32 devices in a mesh: area: 8 (over z, y), tie: 4 (over x, core).
Axes of the slice: x: 2, y: 2, z: 4, core: 2. Of those that a mesh axis runs over, the one named last changes fastest.
Arguments:
- ginv: bfloat16 [128, 1024, 1024], P(('area', 'tie'))
- rhs: float32 [131072, 128], P(('area', 'tie')), may hold values from -6 to 6
- bnd_row: int32 [128, 128], P(('area', 'tie')), may hold values from -1 to 1023, as said below
- bnd_var: int32 [128, 128], P(('area', 'tie')), may hold values from -1 to 2047, as said below
Outputs:
- states: float32 [131072, 128], P(('area', 'tie'))
- consensus: float32 [2048, 128], P(('area', 'tie'))
- dual_value: float32 [16384, 128], P(('area', 'tie'))
The draws below stay inside these ranges and needn't reach their ends.
Inputs may be any that keep to these rules, and one draw needn't show every extreme that they name: `bnd_row`: -1 marks an unused entry slot; the live rows of one area are distinct. `bnd_var`: -1 exactly where bnd_row is -1. Variable v is owned by the device holding rows v of the consensus output, block v // 64. The areas of one device hold at most 4 live entries owned by any one device; in every draw some owner holds exactly 4 from every device.
All inputs are finite; a program needn't handle non-finite values.
Results may differ from the reference program's by a relative error of at most 0.003.
Values sent between devices are 32-bit elements; how exact they have to be, the bound alone decides.
A program may use at most 64 MiB of HBM per device.

```python
import jax
import jax.numpy as jnp
from jax import lax

STATE = 1024
BND = 128
SLOT = 4
VAR_DEV = 64
AREA_DEV = 4
SNAP = 128
ITERS = 4
AREAS = 128
VARS = 2048


def boundary_maps(key):
    device_total = AREAS // AREA_DEV
    entries = AREA_DEV * BND
    hottest = jax.random.randint(jax.random.fold_in(key, 11), (), 0, device_total)
    slot_counts = jax.random.randint(jax.random.fold_in(key, 12), (device_total, device_total), 1, SLOT + 1)
    owner_ids = jnp.arange(device_total, dtype=jnp.int32)
    slot_counts = jnp.where(owner_ids[None, :] == hottest, SLOT, slot_counts)
    slot_live = jnp.arange(SLOT)[None, None, :] < slot_counts[:, :, None]
    local_ids = jax.random.randint(jax.random.fold_in(key, 13), (device_total, device_total, SLOT), 0, VAR_DEV)
    var_slot = jnp.where(slot_live, owner_ids[None, :, None] * VAR_DEV + local_ids, -1)
    var_slot = var_slot.reshape(device_total, device_total * SLOT).astype(jnp.int32)
    perm_keys = jax.random.split(jax.random.fold_in(key, 14), device_total)
    placing = jax.vmap(lambda k: jax.random.permutation(k, entries))(perm_keys)[:, :device_total * SLOT]
    entry_var = jnp.full((device_total, entries), -1, jnp.int32)
    entry_var = entry_var.at[jnp.arange(device_total)[:, None], placing].set(var_slot)
    entry_var = entry_var.reshape(AREAS, BND)
    row_keys = jax.random.split(jax.random.fold_in(key, 15), AREAS)
    row_perm = jax.vmap(lambda k: jax.random.permutation(k, STATE))(row_keys)[:, :BND].astype(jnp.int32)
    entry_row = jnp.where(entry_var >= 0, row_perm, -1).astype(jnp.int32)
    return (entry_row, entry_var)


def draw_bnd_row(key, part):
    return boundary_maps(key)[0]


def draw_bnd_var(key, part):
    return boundary_maps(key)[1]


def draw_ginv(key, part):
    area_keys = jax.random.split(jax.random.fold_in(key, 21), AREAS)

    def one_block(block_key):
        diag_values = jax.random.uniform(jax.random.fold_in(block_key, 7), (STATE,), jnp.float32, 0.3, 0.85)
        noise = jax.random.normal(block_key, (STATE, STATE), jnp.float32)
        return (jnp.diag(diag_values) + 0.3 * noise / STATE ** 0.5).astype(jnp.bfloat16)
    return lax.map(one_block, area_keys)


def block_levels(key, dims, shards, smallest, top_value):
    def one(dim, blocks):
        heights = jax.random.uniform(jax.random.fold_in(jax.random.fold_in(key, 6), dim), (blocks,), jnp.float32, smallest / len(shards), top_value / len(shards))
        return jnp.repeat(jnp.exp(heights), dims[dim] // blocks).reshape((-1,) + (1,) * (len(dims) - dim - 1))

    loudness = one(*shards[0])
    for cut in shards[1:]:
        loudness = loudness * one(*cut)
    return loudness


def scatter_about(stream_key, dims, deviation, most, cuts=(), kind=jnp.bfloat16):
    values = jax.random.normal(stream_key, dims, jnp.float32) * deviation
    if len(cuts) > 0:
        values = block_levels(stream_key, dims, cuts, -0.22, 0.18) * values
    return jnp.clip(values, min=-most, max=most).astype(kind)


def setup_inputs(seed: int = 0) -> dict:
    seeds = jax.random.split(jax.random.key(seed), 5)
    return {
        "ginv": draw_ginv(jax.random.fold_in(seeds[4], 71), 0),
        "rhs": scatter_about(seeds[1], (AREAS * STATE, SNAP), 1.0, 6.0, ((0, 32),), jnp.float32),
        "bnd_row": draw_bnd_row(jax.random.fold_in(seeds[4], 71), 0),
        "bnd_var": draw_bnd_var(jax.random.fold_in(seeds[4], 71), 0),
    }


PENALTY = 1.0


def solve_area(pair):
    return jnp.dot(pair[0], pair[1], preferred_element_type=jnp.float32)


def reference(ginv, rhs, bnd_row, bnd_var):
    areas_total, state_size, _ = ginv.shape
    snap_count = rhs.shape[1]
    active = (bnd_row >= 0).reshape(-1)
    offsets = (jnp.arange(areas_total, dtype=jnp.int32) * state_size)[:, None]
    rows_flat = jnp.where(bnd_row >= 0, offsets + bnd_row, 0).reshape(-1).astype(jnp.int32)
    var_safe = jnp.where(bnd_var >= 0, bnd_var, 0).reshape(-1).astype(jnp.int32)
    counts = jax.ops.segment_sum(active.astype(jnp.float32), var_safe, num_segments=VARS)
    inverse = 1.0 / jnp.maximum(counts, 1.0)
    mask = active[:, None]
    n_entries = rows_flat.shape[0]
    dual_value = jnp.zeros((n_entries, snap_count), jnp.float32)
    agreed = jnp.zeros((n_entries, snap_count), jnp.float32)
    states = None
    consensus = None
    for iteration in range(ITERS):
        shifted = jnp.where(mask, agreed - dual_value, 0.0)
        update = jnp.zeros((areas_total * state_size, snap_count), jnp.float32).at[rows_flat].add(shifted)
        blended = (rhs + PENALTY * update).astype(jnp.bfloat16).reshape(areas_total, state_size, snap_count)
        states = lax.map(solve_area, (ginv, blended)).reshape(areas_total * state_size, snap_count)
        local_part = jnp.where(mask, states[rows_flat] + dual_value, 0.0)
        totals = jax.ops.segment_sum(local_part, var_safe, num_segments=VARS)
        consensus = totals * inverse[:, None]
        agreed = jnp.where(mask, consensus[var_safe], 0.0)
        dual_value = jnp.where(mask, local_part - agreed, 0.0)
    return states, consensus, dual_value
```

```python
import functools

import jax
import jax.numpy as jnp
from jax import lax
from jax.experimental import pallas as pl
from jax.experimental.pallas import tpu as pltpu
from jax.sharding import PartitionSpec as P

SLOT = 4
VAR_DEV = 64
ITERS = 4
PENALTY = 1.0

MESH = pl.DeviceIdType.MESH
F32 = jnp.float32
BF16 = jnp.bfloat16


def mm(a, b):
    return jnp.dot(a, b, preferred_element_type=F32)


def dot_dims(a, b, da, db):
    return lax.dot_general(a, b, (((da,), (db,)), ((), ())), preferred_element_type=F32)


def parts(x):
    high = x.astype(BF16)
    rest = x - high.astype(F32)
    mid = rest.astype(BF16)
    low = (rest - mid.astype(F32)).astype(BF16)
    return high, mid, low


def mm_parts(onehot, x):
    high, mid, low = parts(x)
    return mm(onehot, high) + (mm(onehot, mid) + mm(onehot, low))


def kernel(
    area_n,
    tie_n,
    srow_col,
    srow_lane,
    svar_col,
    g_hbm,
    rhs_hbm,
    states_ref,
    cons_ref,
    dual_ref,
    g_ref,
    rhs_ref,
    pick,
    out_buf,
    in_buf,
    rhs_b,
    y_base,
    g_bb,
    load_sem,
    send_sem,
    recv_sem,
):
    devices = area_n * tie_n
    area_dev, state_size, _ = g_ref.shape
    cap = devices * SLOT
    snap = dual_ref.shape[1]
    me_a, me_t = lax.axis_index("area"), lax.axis_index("tie")
    me = me_a * tie_n + me_t

    def peer_of(k):
        peer = lax.rem(me + k, devices)
        return peer, (peer // tie_n, lax.rem(peer, tie_n))

    barrier = pltpu.get_barrier_semaphore()

    @pl.loop(1, devices)
    def _(k):
        _, device = peer_of(k)
        pl.semaphore_signal(barrier, inc=1, device_id=device, device_id_type=MESH)

    def g_load(a):
        return pltpu.make_async_copy(g_hbm.at[a], g_ref.at[a], load_sem.at[0, a])

    def rhs_load(a):
        return pltpu.make_async_copy(rhs_hbm.at[a], rhs_ref.at[a], load_sem.at[1, a])

    for a in range(area_dev):
        g_load(a).start()
        rhs_load(a).start()

    def send(phase, value):
        out_buf[phase] = value.reshape(devices, SLOT, snap)
        in_buf[phase, me] = out_buf[phase, me]

        @pl.loop(1, devices)
        def _(k):
            peer, device = peer_of(k)
            pltpu.make_async_remote_copy(
                src_ref=out_buf.at[phase, peer],
                dst_ref=in_buf.at[phase, me],
                send_sem=send_sem.at[phase],
                recv_sem=recv_sem.at[phase],
                device_id=device,
                device_id_type=MESH,
            ).start()

    def receive(phase):
        span = in_buf.at[phase, pl.ds(0, devices - 1)]
        pltpu.make_async_copy(span, span, recv_sem.at[phase]).wait()
        return in_buf[phase].reshape(cap, snap)

    lane = lax.broadcasted_iota(jnp.int32, (cap, snap), 1)
    member_out = (svar_col[...] == lane).astype(F32)
    pl.semaphore_wait(barrier, devices - 1)
    send(0, member_out)

    rhs_b[...] = jnp.zeros_like(rhs_b)
    y_base[...] = jnp.zeros_like(y_base)
    g_bb[...] = jnp.zeros_like(g_bb)

    @pl.loop(0, area_dev)
    def _(a):
        column = lax.broadcasted_iota(jnp.int32, (cap, state_size), 1) + a * state_size
        chosen = (jnp.broadcast_to(srow_col[:, :1], (cap, state_size)) == column).astype(F32)
        chosen = chosen.astype(BF16)
        line = lax.broadcasted_iota(jnp.int32, (state_size, cap), 0) + a * state_size
        pick[a] = (
            (jnp.broadcast_to(srow_lane[:1, :], (state_size, cap)) == line)
            .astype(F32)
            .astype(BF16)
        )
        rhs_load(a).wait()
        high, mid, low = parts(rhs_ref[a])
        rhs_b[...] += mm(chosen, high) + (mm(chosen, mid) + mm(chosen, low))
        g_load(a).wait()
        rows = mm(chosen, g_ref[a]).astype(BF16)
        y_base[...] += mm(rows, high)
        g_bb[...] += mm(rows, pick[a])

    inner = g_bb[...].astype(BF16)
    own = rhs_b[...]
    first = y_base[...]
    steady = first - mm(inner, own.astype(BF16))

    member = receive(0).astype(BF16)
    same = dot_dims(member, member, 1, 1)
    share = 1.0 / jnp.maximum(jnp.sum(same, axis=1, keepdims=True), 1.0)
    same = same.astype(BF16)
    dual = jnp.zeros((cap, snap), F32)
    update = jnp.zeros((cap, snap), F32)
    for it in range(ITERS):
        if it == 0:
            local = first
        else:
            blended = (own + PENALTY * update).astype(BF16)
            local = steady + mm(inner, blended) + dual
        send(1 + 2 * it, local)
        if it == ITERS - 1:
            moved = parts(update)

            @pl.loop(0, area_dev)
            def _(a):
                scattered = mm(pick[a], moved[0]) + (mm(pick[a], moved[1]) + mm(pick[a], moved[2]))
                mixed = (rhs_ref[a] + PENALTY * scattered).astype(BF16)
                states_ref[a] = mm(g_ref[a], mixed)

        incoming = receive(1 + 2 * it)
        send(2 + 2 * it, mm_parts(same, incoming) * share)
        if it == ITERS - 1:
            high, mid, low = parts(incoming)
            totals = dot_dims(member, high, 0, 0) + (
                dot_dims(member, mid, 0, 0) + dot_dims(member, low, 0, 0)
            )
            counts = dot_dims(member, jnp.ones((cap, snap), BF16), 0, 0)
            consensus = totals * (1.0 / jnp.maximum(counts, 1.0))
            cons_ref[...] = consensus[: cons_ref.shape[0]]
        agreed = receive(2 + 2 * it)
        dual = local - agreed
        update = agreed - dual
    dual_ref[...] = dual

    for phase in range(1 + 2 * ITERS):
        span = out_buf.at[phase, pl.ds(0, devices - 1)]
        pltpu.make_async_copy(span, span, send_sem.at[phase]).wait()


def on_device(ginv, rhs, bnd_row, bnd_var):
    area_dev, state_size, _ = ginv.shape
    snap = rhs.shape[1]
    bound_size = bnd_row.shape[1]
    entries = area_dev * bound_size
    area_n = lax.axis_size("area")
    tie_n = lax.axis_size("tie")
    devices = area_n * tie_n
    cap = devices * SLOT
    row_flat = bnd_row.reshape(entries)
    var_flat = bnd_var.reshape(entries)
    active = row_flat >= 0
    order = jnp.arange(entries, dtype=jnp.int32)
    state_row = (order // bound_size) * state_size + row_flat
    owners = jnp.where(active, var_flat // VAR_DEV, devices)
    owned = owners[:, None] == jnp.arange(devices, dtype=jnp.int32)[None, :]
    earlier = (order[:, None] > order[None, :]).astype(BF16)
    before = mm(earlier, owned.astype(BF16))
    placed = jnp.sum(jnp.where(owned, before, 0.0), axis=1).astype(jnp.int32)
    slot = jnp.where(active, owners * SLOT + placed, -1)
    slots = jnp.arange(cap, dtype=jnp.int32)
    held = slots[:, None] == slot[None, :]
    srow = jnp.sum(jnp.where(held, (state_row + 1)[None, :], 0), axis=1) - 1
    svar = jnp.sum(jnp.where(held, (var_flat % VAR_DEV + 1)[None, :], 0), axis=1) - 1
    phases = 1 + 2 * ITERS
    vmem = pl.BlockSpec(memory_space=pltpu.VMEM)
    hbm = pl.BlockSpec(memory_space=pl.ANY)
    states, consensus, dual = pl.pallas_call(
        functools.partial(kernel, area_n, tie_n),
        out_shape=(
            jax.ShapeDtypeStruct((area_dev, state_size, snap), F32),
            jax.ShapeDtypeStruct((VAR_DEV, snap), F32),
            jax.ShapeDtypeStruct((cap, snap), F32),
        ),
        in_specs=[vmem, vmem, vmem, hbm, hbm],
        out_specs=(vmem, vmem, vmem),
        scratch_shapes=[
            pltpu.VMEM(ginv.shape, BF16),
            pltpu.VMEM((area_dev, state_size, snap), F32),
            pltpu.VMEM((area_dev, state_size, cap), BF16),
            pltpu.VMEM((phases, devices, SLOT, snap), F32),
            pltpu.VMEM((phases, devices, SLOT, snap), F32),
            pltpu.VMEM((cap, snap), F32),
            pltpu.VMEM((cap, snap), F32),
            pltpu.VMEM((cap, cap), F32),
            pltpu.SemaphoreType.DMA((2, area_dev)),
            pltpu.SemaphoreType.DMA((phases,)),
            pltpu.SemaphoreType.DMA((phases,)),
        ],
        compiler_params=pltpu.CompilerParams(
            collective_id=0, has_side_effects=True, vmem_limit_bytes=48 * 1024 * 1024
        ),
        name="admm",
    )(
        jnp.broadcast_to(srow[:, None], (cap, snap)),
        jnp.broadcast_to(srow[None, :], (8, cap)),
        jnp.broadcast_to(svar[:, None], (cap, snap)),
        ginv,
        rhs.reshape(area_dev, state_size, snap),
    )
    spread = (slot[:, None] == slots[None, :]).astype(F32)
    dual = jnp.dot(spread, dual, precision=lax.Precision.HIGHEST)
    return (states.reshape(area_dev * state_size, snap), consensus, dual)


def solution(mesh):
    both = ("area", "tie")
    in_specs = (P(both, None, None), P(both, None), P(both, None), P(both, None))
    out_specs = (P(both, None), P(both, None), P(both, None))
    return jax.shard_map(
        on_device, mesh=mesh, in_specs=in_specs, out_specs=out_specs, check_vma=False
    )
```

```python
import functools

import jax
import jax.numpy as jnp
from jax import lax
from jax.experimental import pallas as pl
from jax.experimental.pallas import tpu as pltpu
from jax.sharding import PartitionSpec as P

SLOT = 4
VAR_DEV = 64
ITERS = 4
PENALTY = 1.0

MESH = pl.DeviceIdType.MESH
F32 = jnp.float32
BF16 = jnp.bfloat16


def mm(a, b):
    return jnp.dot(a, b, preferred_element_type=F32)


def dot_dims(a, b, da, db):
    return lax.dot_general(a, b, (((da,), (db,)), ((), ())), preferred_element_type=F32)


def parts(x):
    high = x.astype(BF16)
    rest = x - high.astype(F32)
    mid = rest.astype(BF16)
    low = (rest - mid.astype(F32)).astype(BF16)
    return high, mid, low


def mm_parts(onehot, x):
    high, mid, low = parts(x)
    return mm(onehot, high) + (mm(onehot, mid) + mm(onehot, low))


def kernel(
    area_n,
    tie_n,
    srow_col,
    srow_lane,
    svar_col,
    g_hbm,
    rhs_hbm,
    states_ref,
    cons_ref,
    dual_ref,
    g_ref,
    rhs_ref,
    pick,
    out_buf,
    in_buf,
    rhs_b,
    y_base,
    g_bb,
    load_sem,
    send_sem,
    recv_sem,
):
    devices = area_n * tie_n
    area_dev, state_size, _ = g_ref.shape
    cap = devices * SLOT
    snap = dual_ref.shape[1]
    me_a, me_t = lax.axis_index("area"), lax.axis_index("tie")
    me = me_a * tie_n + me_t

    blocks = 4 if devices % 4 == 0 else 1
    block = devices // blocks
    me_block, me_in = me // block, lax.rem(me, block)
    upper = 2 * me_block >= blocks
    turned = jnp.where(upper, me_block, blocks - 1 - me_block)

    def peer_of(k):
        peer = lax.rem(me + k, devices)
        return peer, (peer // tie_n, lax.rem(peer, tie_n))

    barrier = pltpu.get_barrier_semaphore()

    @pl.loop(1, devices)
    def _(k):
        _, device = peer_of(k)
        pl.semaphore_signal(barrier, inc=1, device_id=device, device_id_type=MESH)

    def g_load(a):
        return pltpu.make_async_copy(g_hbm.at[a], g_ref.at[a], load_sem.at[0, a])

    def rhs_load(a):
        return pltpu.make_async_copy(rhs_hbm.at[a], rhs_ref.at[a], load_sem.at[1, a])

    for a in range(area_dev):
        g_load(a).start()
        rhs_load(a).start()

    def send(phase, value):
        out_buf[phase] = value.reshape(devices, SLOT, snap)
        in_buf[phase, me] = out_buf[phase, me]

        def post(peer):
            pltpu.make_async_remote_copy(
                src_ref=out_buf.at[phase, peer],
                dst_ref=in_buf.at[phase, me],
                send_sem=send_sem.at[phase],
                recv_sem=recv_sem.at[phase],
                device_id=(peer // tie_n, lax.rem(peer, tie_n)),
                device_id_type=MESH,
            ).start()

        @pl.loop(0, blocks - 1)
        def _(b):
            placed = b + jnp.where(b >= turned, 1, 0)
            base = jnp.where(upper, placed, blocks - 1 - placed) * block
            for i in range(block):
                post(base + lax.rem(me_in + i, block))

        for i in range(1, block):
            post(me_block * block + lax.rem(me_in + i, block))

    def receive(phase):
        span = in_buf.at[phase, pl.ds(0, devices - 1)]
        pltpu.make_async_copy(span, span, recv_sem.at[phase]).wait()
        return in_buf[phase].reshape(cap, snap)

    lane = lax.broadcasted_iota(jnp.int32, (cap, snap), 1)
    member_out = (svar_col[...] == lane).astype(F32)
    pl.semaphore_wait(barrier, devices - 1)
    send(0, member_out)

    rhs_b[...] = jnp.zeros_like(rhs_b)
    y_base[...] = jnp.zeros_like(y_base)
    g_bb[...] = jnp.zeros_like(g_bb)

    @pl.loop(0, area_dev)
    def _(a):
        column = lax.broadcasted_iota(jnp.int32, (cap, state_size), 1) + a * state_size
        chosen = (jnp.broadcast_to(srow_col[:, :1], (cap, state_size)) == column).astype(F32)
        chosen = chosen.astype(BF16)
        line = lax.broadcasted_iota(jnp.int32, (state_size, cap), 0) + a * state_size
        pick[a] = (
            (jnp.broadcast_to(srow_lane[:1, :], (state_size, cap)) == line)
            .astype(F32)
            .astype(BF16)
        )
        rhs_load(a).wait()
        high, mid, low = parts(rhs_ref[a])
        rhs_b[...] += mm(chosen, high) + (mm(chosen, mid) + mm(chosen, low))
        g_load(a).wait()
        rows = mm(chosen, g_ref[a]).astype(BF16)
        y_base[...] += mm(rows, high)
        g_bb[...] += mm(rows, pick[a])

    inner = g_bb[...].astype(BF16)
    own = rhs_b[...]
    first = y_base[...]
    steady = first - mm(inner, own.astype(BF16))

    member = receive(0).astype(BF16)
    same = dot_dims(member, member, 1, 1)
    share = 1.0 / jnp.maximum(jnp.sum(same, axis=1, keepdims=True), 1.0)
    same = same.astype(BF16)
    dual = jnp.zeros((cap, snap), F32)
    update = jnp.zeros((cap, snap), F32)
    for it in range(ITERS):
        if it == 0:
            local = first
        else:
            blended = (own + PENALTY * update).astype(BF16)
            local = steady + mm(inner, blended) + dual
        send(1 + 2 * it, local)
        if it == ITERS - 1:
            moved = parts(update)

            @pl.loop(0, area_dev)
            def _(a):
                scattered = mm(pick[a], moved[0]) + (mm(pick[a], moved[1]) + mm(pick[a], moved[2]))
                mixed = (rhs_ref[a] + PENALTY * scattered).astype(BF16)
                states_ref[a] = mm(g_ref[a], mixed)

        incoming = receive(1 + 2 * it)
        send(2 + 2 * it, mm_parts(same, incoming) * share)
        if it == ITERS - 1:
            high, mid, low = parts(incoming)
            totals = dot_dims(member, high, 0, 0) + (
                dot_dims(member, mid, 0, 0) + dot_dims(member, low, 0, 0)
            )
            counts = dot_dims(member, jnp.ones((cap, snap), BF16), 0, 0)
            consensus = totals * (1.0 / jnp.maximum(counts, 1.0))
            cons_ref[...] = consensus[: cons_ref.shape[0]]
        agreed = receive(2 + 2 * it)
        dual = local - agreed
        update = agreed - dual
    dual_ref[...] = dual

    for phase in range(1 + 2 * ITERS):
        span = out_buf.at[phase, pl.ds(0, devices - 1)]
        pltpu.make_async_copy(span, span, send_sem.at[phase]).wait()


def on_device(ginv, rhs, bnd_row, bnd_var):
    area_dev, state_size, _ = ginv.shape
    snap = rhs.shape[1]
    bound_size = bnd_row.shape[1]
    entries = area_dev * bound_size
    area_n = lax.axis_size("area")
    tie_n = lax.axis_size("tie")
    devices = area_n * tie_n
    cap = devices * SLOT
    row_flat = bnd_row.reshape(entries)
    var_flat = bnd_var.reshape(entries)
    active = row_flat >= 0
    order = jnp.arange(entries, dtype=jnp.int32)
    state_row = (order // bound_size) * state_size + row_flat
    owners = jnp.where(active, var_flat // VAR_DEV, devices)
    owned = owners[:, None] == jnp.arange(devices, dtype=jnp.int32)[None, :]
    earlier = (order[:, None] > order[None, :]).astype(BF16)
    before = mm(earlier, owned.astype(BF16))
    placed = jnp.sum(jnp.where(owned, before, 0.0), axis=1).astype(jnp.int32)
    slot = jnp.where(active, owners * SLOT + placed, -1)
    slots = jnp.arange(cap, dtype=jnp.int32)
    held = slots[:, None] == slot[None, :]
    srow = jnp.sum(jnp.where(held, (state_row + 1)[None, :], 0), axis=1) - 1
    svar = jnp.sum(jnp.where(held, (var_flat % VAR_DEV + 1)[None, :], 0), axis=1) - 1
    phases = 1 + 2 * ITERS
    vmem = pl.BlockSpec(memory_space=pltpu.VMEM)
    hbm = pl.BlockSpec(memory_space=pl.ANY)
    states, consensus, dual = pl.pallas_call(
        functools.partial(kernel, area_n, tie_n),
        out_shape=(
            jax.ShapeDtypeStruct((area_dev, state_size, snap), F32),
            jax.ShapeDtypeStruct((VAR_DEV, snap), F32),
            jax.ShapeDtypeStruct((cap, snap), F32),
        ),
        in_specs=[vmem, vmem, vmem, hbm, hbm],
        out_specs=(vmem, vmem, vmem),
        scratch_shapes=[
            pltpu.VMEM(ginv.shape, BF16),
            pltpu.VMEM((area_dev, state_size, snap), F32),
            pltpu.VMEM((area_dev, state_size, cap), BF16),
            pltpu.VMEM((phases, devices, SLOT, snap), F32),
            pltpu.VMEM((phases, devices, SLOT, snap), F32),
            pltpu.VMEM((cap, snap), F32),
            pltpu.VMEM((cap, snap), F32),
            pltpu.VMEM((cap, cap), F32),
            pltpu.SemaphoreType.DMA((2, area_dev)),
            pltpu.SemaphoreType.DMA((phases,)),
            pltpu.SemaphoreType.DMA((phases,)),
        ],
        compiler_params=pltpu.CompilerParams(
            collective_id=0, has_side_effects=True, vmem_limit_bytes=48 * 1024 * 1024
        ),
        name="admm",
    )(
        jnp.broadcast_to(srow[:, None], (cap, snap)),
        jnp.broadcast_to(srow[None, :], (8, cap)),
        jnp.broadcast_to(svar[:, None], (cap, snap)),
        ginv,
        rhs.reshape(area_dev, state_size, snap),
    )
    spread = (slot[:, None] == slots[None, :]).astype(F32)
    dual = jnp.dot(spread, dual, precision=lax.Precision.HIGHEST)
    return (states.reshape(area_dev * state_size, snap), consensus, dual)


def solution(mesh):
    both = ("area", "tie")
    in_specs = (P(both, None, None), P(both, None), P(both, None), P(both, None))
    out_specs = (P(both, None), P(both, None), P(both, None))
    return jax.shard_map(
        on_device, mesh=mesh, in_specs=in_specs, out_specs=out_specs, check_vma=False
    )
```
